256 devices in a mesh: expert: 8 (over y, z_lo), tensor: 32 (over z_hi, x, core).
Axes of the slice: x: 4, y: 4, z: 8 (z_hi: 4, z_lo: 2; z = z_hi * 2 + z_lo), core: 2. Of those that a mesh axis runs over, the one named last changes fastest.
Arguments:
- tokens: bfloat16 [2048, 6144], P(('expert', 'tensor')), may hold values from -6 to 6
- expert_ids: int32 [2048, 2], P(('expert', 'tensor')), may hold values from 0 to 7, all different within a row; in each aligned block of 8 rows (0 to 7, 8 to 15, ...) at most 3 rows name the same one
- gates: float32 [2048, 2], P(('expert', 'tensor')), may hold values from 0.2 to 1
- w_gate: bfloat16 [8, 6144, 8192], P('expert', None, 'tensor'), may hold values from -0.078125 to 0.078125
- w_up: bfloat16 [8, 6144, 8192], P('expert', None, 'tensor'), may hold values from -0.078125 to 0.078125
- w_down: bfloat16 [8, 8192, 6144], P('expert', 'tensor'), may hold values from -0.0625 to 0.0625
Outputs:
- mixed: bfloat16 [2048, 6144], P(('expert', 'tensor'))
The draws below stay inside these ranges and needn't reach their ends.
Inputs may be any that keep to these rules, and one draw needn't show every extreme that they name: `expert_ids`: each token names 2 different experts. Among the tokens of one device (aligned blocks of 8 rows) no expert is named more than 3 times, a bound that some expert reaches in every block.
All inputs are finite; a program needn't handle non-finite values.
Results may differ from the reference program's by a relative error of at most 0.02.
Values may be sent and summed in bfloat16 or wider, within the bound.
No kernel may reach another device: no remote copies, remote signals or barrier semaphores. Data moves between devices by JAX's collectives and lax.ppermute only.
A program may use at most 128 MiB of HBM per device.

```python
import math
import jax
import jax.numpy as jnp
import numpy as np
from jax import lax

D = 6144
FF = 8192
EXPERTS = 8
TOPK = 2
TOK_DEV = 8
CAP = 3
TOKENS = 2048
N_EXPERT = 8
N_TENSOR = 32


def level_of(key, dims, split, least, top_value):
    def one(axis_at, parts):
        draws = jax.random.uniform(jax.random.fold_in(jax.random.fold_in(key, 6), axis_at), (parts,), jnp.float32, least / len(split), top_value / len(split))
        return jnp.repeat(jnp.exp(draws), dims[axis_at] // parts).reshape((-1,) + (1,) * (len(dims) - axis_at - 1))

    gain = one(*split[0])
    for cut in split[1:]:
        gain = gain * one(*cut)
    return gain


def routed_block(own_key, own, number, rows, count, top, bound, skew):
    order = jax.random.permutation(own_key, count)
    heavy_load, usual = shares(count, rows * top, bound, skew, True), shares(count, rows * top, bound, skew, False)
    places = jnp.arange(count)

    def named(lengths, turn):
        used = int((lengths > 0).sum())
        fixed = max(1, used // 4)
        shifted = fixed + (places - fixed + turn * (used - fixed)) % max(1, count - fixed)
        return jnp.zeros((count,), jnp.int32).at[order[jnp.where(places < fixed, places, shifted)]].set(jnp.asarray(lengths, jnp.int32))

    lengths = jnp.where(number % 4 == 0, named(heavy_load, number // 4), named(usual, number - number // 4 - 1))
    mixed = jax.random.permutation(jax.random.fold_in(own, 3), count)
    giver, sink = mixed[0:count // 2 * 2:2], mixed[1:count // 2 * 2:2]
    room = jnp.minimum(lengths[giver] - 1, bound - lengths[sink]) // 2
    room = jnp.where((giver == order[0]) | (sink == order[0]) | (lengths[sink] == 0), 0, jnp.maximum(room, 0))
    shifted = jax.random.randint(jax.random.fold_in(own, 4), (count // 2,), 0, 1 << 20) % (room + 1)
    lengths = lengths.at[giver].add(-shifted).at[sink].add(shifted)
    labels = jnp.searchsorted(jnp.cumsum(lengths), jnp.arange(rows * top), side="right").astype(jnp.int32)
    table = labels.reshape(top, rows).T
    table = table[jax.random.permutation(jax.random.fold_in(own, 1), rows)]
    turn = jax.random.randint(jax.random.fold_in(own, 2), (rows, 1), 0, top)
    return jnp.take_along_axis(table, (jnp.arange(top)[None, :] + turn) % top, axis=1)


def shares(count, total, most, skew, full):
    portions = [(1 << 20) // math.isqrt(grade ** skew) + 1 for grade in range(1, count + 1)]
    largest = most if full else min(most, max(-(-total // count), total * portions[0] // sum(portions)))
    least = 1 if total - largest >= count - 1 else 0
    counts, rest = [largest] + [least] * (count - 1), total - largest - least * (count - 1)
    while rest > 0:
        free = [i for i in range(1, count) if counts[i] < largest] or [i for i in range(1, count) if counts[i] < most]
        pool, budget = sum([portions[i] for i in free]), rest
        for i in free:
            addition = min(most - counts[i], max(1, budget * portions[i] // pool), rest)
            counts[i] = counts[i] + addition
            rest = rest - addition
    return np.array(counts)


def scatter_about(rng, shape, scale, bound, cuts=(), held_as=jnp.bfloat16):
    result = scale * jax.random.normal(rng, shape, jnp.float32)
    if cuts:
        result = result * level_of(rng, shape, cuts, -0.22, 0.18)
    return jnp.clip(result, -bound, bound).astype(held_as)


def setup_inputs(seed: int = 0) -> dict:
    arg_keys = jax.random.split(jax.random.key(seed), 7)
    tokens = scatter_about(arg_keys[0], (TOKENS, D), 1.0, 6.0, ((0, 256),))
    expert_ids_keys = jax.random.split(jax.random.fold_in(arg_keys[1], 1), TOKENS // TOK_DEV)
    expert_ids_turns = jax.random.permutation(jax.random.fold_in(arg_keys[1], 3), TOKENS // TOK_DEV)
    expert_ids = jax.vmap(lambda own, number: routed_block(jax.random.fold_in(arg_keys[1], 2), own, number, TOK_DEV, EXPERTS, TOPK, CAP, 2))(expert_ids_keys, expert_ids_turns).reshape((TOKENS, TOPK))
    gates = jnp.clip(0.2 + 0.8 * jax.random.uniform(arg_keys[2], (TOKENS, TOPK), jnp.float32) ** level_of(arg_keys[2], (TOKENS, TOPK), ((0, 256),), -0.2, 0.2), 0.2, 1.0)
    w_gate = scatter_about(arg_keys[3], (EXPERTS, D, FF), D ** -0.5, 0.078125, ((0, 8), (2, 32)))
    w_up = scatter_about(arg_keys[4], (EXPERTS, D, FF), D ** -0.5, 0.078125, ((0, 8), (2, 32)))
    w_down = scatter_about(arg_keys[5], (EXPERTS, FF, D), FF ** -0.5, 0.0625, ((0, 8), (1, 32)))
    return dict(tokens=tokens, expert_ids=expert_ids, gates=gates, w_gate=w_gate, w_up=w_up, w_down=w_down)


def route_places(ids):
    flat = ids.reshape(-1).astype(jnp.int32)
    onehot = (flat[:, None] == jnp.arange(EXPERTS, dtype=jnp.int32)[None, :]).astype(jnp.int32)
    before = jnp.cumsum(onehot, axis=0) - onehot
    slot = jnp.sum(before * onehot, axis=1)
    return (flat * CAP + slot).astype(jnp.int32)


def dispatch_block(rows, places):
    picker = (jnp.arange(EXPERTS * CAP, dtype=jnp.int32)[:, None] == places[None, :]).astype(jnp.bfloat16)
    doubled = jnp.repeat(rows, TOPK, axis=0)
    return jnp.dot(picker, doubled, preferred_element_type=jnp.float32).astype(jnp.bfloat16)


def combine_block(gate_rows, places, results):
    weights = (jnp.arange(EXPERTS * CAP, dtype=jnp.int32)[None, :] == places[:, None]).astype(jnp.float32)
    weights = weights * gate_rows.reshape(-1)[:, None]
    weights = jnp.sum(weights.reshape(TOK_DEV, TOPK, EXPERTS * CAP), axis=1)
    return jnp.dot(weights, results.astype(jnp.float32), precision=lax.Precision.HIGHEST).astype(jnp.bfloat16)


def expert_ffn(item):
    rows, gate_matrix, up_matrix, down_matrix = item
    shard = FF // N_TENSOR
    gate_act = jnp.dot(rows, gate_matrix, preferred_element_type=jnp.float32)
    up_act = jnp.dot(rows, up_matrix, preferred_element_type=jnp.float32)
    hidden = (jax.nn.silu(gate_act) * up_act).astype(jnp.bfloat16)
    pieces = hidden.reshape(rows.shape[0], N_TENSOR, shard).transpose(1, 0, 2)
    downs = down_matrix.reshape(N_TENSOR, shard, D)

    def add_part(total, pair):
        part = jnp.dot(pair[0], pair[1], preferred_element_type=jnp.float32).astype(jnp.bfloat16)
        part = lax.optimization_barrier(part)
        return total + part.astype(jnp.float32), None

    total, _ = lax.scan(add_part, jnp.zeros((rows.shape[0], D), jnp.float32), (pieces, downs))
    return total.astype(jnp.bfloat16)


def reference(tokens, expert_ids, gates, w_gate, w_up, w_down):
    blocks = N_EXPERT * N_TENSOR
    token_blocks = tokens.reshape(blocks, TOK_DEV, D)
    id_blocks = expert_ids.reshape(blocks, TOK_DEV, TOPK)
    gate_blocks = gates.reshape(blocks, TOK_DEV, TOPK)
    places = jax.vmap(route_places)(id_blocks)
    buffers = jax.vmap(dispatch_block)(token_blocks, places)
    by_expert = buffers.reshape(blocks, EXPERTS, CAP, D).transpose(1, 0, 2, 3).reshape(EXPERTS, blocks * CAP, D)
    outputs = lax.map(expert_ffn, (by_expert, w_gate, w_up, w_down))
    home = outputs.reshape(EXPERTS, blocks, CAP, D).transpose(1, 0, 2, 3).reshape(blocks, EXPERTS * CAP, D)
    mixed = jax.vmap(combine_block)(gate_blocks, places, home)
    return mixed.reshape(blocks * TOK_DEV, D)
```

```python
import jax
import jax.numpy as jnp
from jax import lax
from jax.experimental import pallas as pl
from jax.experimental.pallas import tpu as pltpu
from jax.sharding import Mesh, PartitionSpec as P

EXPERTS = 8
TOPK = 2
CAP = 3

AXES = ("y", "w", "z", "x", "c")
SIZES = (4, 2, 4, 4, 2)
EXPERT = ("y", "w")
TENSOR = ("z", "x", "c")


def put(a, axis, k):
    n = SIZES[AXES.index(axis)]
    return lax.ppermute(a, axis, [(i, (i + k) % n) for i in range(n)])


def get(a, axis, k):
    return put(a, axis, -k)


def route_places(ids):
    flat = ids.reshape(-1)
    onehot = (flat[:, None] == jnp.arange(EXPERTS, dtype=jnp.int32)[None, :]).astype(jnp.int32)
    before = jnp.cumsum(onehot, axis=0) - onehot
    slot = jnp.sum(before * onehot, axis=1)
    return flat * CAP + slot


def gate_up(xs, wg, wu):
    rows = [x.shape[0] for x in xs]
    depth, width = wg[0].shape
    block = 1024
    steps = depth // block
    total = sum(rows)
    n = len(xs)

    def kernel(*refs):
        x_refs, (wg0, wg1, wu0, wu1), h_ref = refs[:n], refs[n : n + 4], refs[n + 4]
        g_acc, u_acc = refs[n + 5 :]
        k = pl.program_id(0)
        x = jnp.concatenate([r[...] for r in x_refs], axis=0)

        @pl.when(k == 0)
        def _():
            g_acc[...] = jnp.zeros_like(g_acc)
            u_acc[...] = jnp.zeros_like(u_acc)

        for j, (g_w, u_w) in enumerate(((wg0, wu0), (wg1, wu1))):
            cols = slice(j * width, (j + 1) * width)
            g_acc[:, cols] += jnp.dot(x, g_w[...], preferred_element_type=jnp.float32)
            u_acc[:, cols] += jnp.dot(x, u_w[...], preferred_element_type=jnp.float32)

        @pl.when(k == steps - 1)
        def _():
            g = g_acc[...]
            h_ref[...] = (g / (1.0 + jnp.exp(-g)) * u_acc[...]).astype(jnp.bfloat16)

    return pl.pallas_call(
        kernel,
        grid=(steps,),
        in_specs=[pl.BlockSpec((r, block), lambda k: (0, k)) for r in rows]
        + [pl.BlockSpec((block, width), lambda k: (k, 0))] * 4,
        out_specs=pl.BlockSpec((total, 2 * width), lambda k: (0, 0)),
        out_shape=jax.ShapeDtypeStruct((total, 2 * width), jnp.bfloat16),
        scratch_shapes=[pltpu.VMEM((total, 2 * width), jnp.float32)] * 2,
        compiler_params=pltpu.CompilerParams(dimension_semantics=("arbitrary",)),
        cost_estimate=pl.CostEstimate(
            flops=8 * total * depth * width,
            bytes_accessed=2 * (total * depth + 4 * depth * width + 2 * total * width),
            transcendentals=2 * total * width,
        ),
    )(*xs, *wg, *wu)


def down(h, wd, rows):
    total, both = h.shape
    width, depth = wd[0].shape
    block = 1024
    n = len(rows)

    def kernel(h_ref, wd0, wd1, *out_refs):
        o = jnp.dot(h_ref[:, :width], wd0[...], preferred_element_type=jnp.float32)
        o += jnp.dot(h_ref[:, width:], wd1[...], preferred_element_type=jnp.float32)
        o = o.astype(jnp.bfloat16)
        at = 0
        for r, ref in zip(rows, out_refs):
            ref[...] = o[at : at + r]
            at += r

    return pl.pallas_call(
        kernel,
        grid=(depth // block,),
        in_specs=[pl.BlockSpec((total, both), lambda k: (0, 0))]
        + [pl.BlockSpec((width, block), lambda k: (0, k))] * 2,
        out_specs=[pl.BlockSpec((r, block), lambda k: (0, k)) for r in rows],
        out_shape=[jax.ShapeDtypeStruct((r, depth), jnp.bfloat16) for r in rows],
        compiler_params=pltpu.CompilerParams(dimension_semantics=("arbitrary",)),
        cost_estimate=pl.CostEstimate(
            flops=4 * total * depth * width,
            bytes_accessed=2 * (2 * depth * width + total * depth + 2 * total * width),
            transcendentals=0,
        ),
    )(h, *wd)


def add(*terms):
    return sum(t.astype(jnp.float32) for t in terms).astype(jnp.bfloat16)


WAY = {0: 1, 1: 1, -1: -1, 2: -1}
XS = (0, 1, -1, 2)


def body(tokens, expert_ids, gates, w_gate, w_up, w_down):
    width = tokens.shape[1]
    tok_count = tokens.shape[0]
    wg, wu, wd = (
        (w[0], put(w, "c", 1)[0]) for w in (w_gate, w_up, w_down)
    )
    places = route_places(expert_ids)
    picker = (jnp.arange(EXPERTS * CAP, dtype=jnp.int32)[:, None] == places[None, :]).astype(
        jnp.bfloat16
    )
    doubled = jnp.repeat(tokens, TOPK, axis=0)
    buffer = jnp.dot(picker, doubled, preferred_element_type=jnp.float32).astype(jnp.bfloat16)
    arrived = lax.all_to_all(
        buffer.reshape(EXPERTS, CAP, width), EXPERT, split_axis=0, concat_axis=0, tiled=True
    )
    own = arrived.reshape(EXPERTS * CAP, width)

    held = {(0, 0): own}
    for z in (1, -1, 2):
        held[0, z] = get(own, "z", z)
    for z in (0, 1, -1, 2):
        for x in (1, -1):
            held[x, z] = get(held[0, z], "x", x)
        way = WAY[z]
        held[2, z] = get(held[way, z], "x", way)

    part = {}
    for zs in ((0, 1, -1), (2,)):
        keys = [(x, z) for z in zs for x in XS]
        xs = [held[k] for k in keys]
        outs = down(gate_up(xs, wg, wu), wd, [x.shape[0] for x in xs])
        part.update(zip(keys, outs))

    summed = {}
    for z in (1, -1, 2, 0):
        d = WAY[z]
        far = put(part[2, z], "x", d)
        near = put(part[-d, z], "x", -d)
        both = put(add(part[d, z], far), "x", d)
        summed[z] = (part[0, z], near, both)
    sent = [put(add(*summed[z]), "z", z) for z in (1, -1, 2)]
    results = add(*summed[0], *sent)

    returned = lax.all_to_all(
        results.reshape(EXPERTS, CAP, width), EXPERT, split_axis=0, concat_axis=0, tiled=True
    )
    results_flat = returned.reshape(EXPERTS * CAP, width)
    weights = (jnp.arange(EXPERTS * CAP, dtype=jnp.int32)[None, :] == places[:, None]).astype(
        jnp.float32
    )
    weights = weights * gates.reshape(-1)[:, None]
    weights = jnp.sum(weights.reshape(tok_count, TOPK, EXPERTS * CAP), axis=1)
    mixed = jnp.dot(weights, results_flat.astype(jnp.float32), precision=lax.Precision.HIGHEST)
    return mixed.astype(jnp.bfloat16)


def solution(mesh):
    fine = Mesh(mesh.devices.reshape(SIZES), AXES)
    tokens = P(EXPERT + TENSOR, None)
    return jax.shard_map(
        body,
        mesh=fine,
        in_specs=(
            tokens,
            tokens,
            tokens,
            P(EXPERT, None, TENSOR),
            P(EXPERT, None, TENSOR),
            P(EXPERT, TENSOR, None),
        ),
        out_specs=tokens,
        check_vma=False,
    )
```
